32 devices in a mesh: gx: 4 (over x, core), gy: 8 (over z, y).
Axes of the slice: x: 2, y: 2, z: 4, core: 2. Of those that a mesh axis runs over, the one named last changes fastest.
Arguments:
- atm_fields: bfloat16 [196608, 128], P(('gx', 'gy')), may hold values from -6 to 6
- atm_pos: int32 [768], replicated, may hold values from 0 to 767, as said below
- tile_src: int32 [5120], P(('gx', 'gy')), may hold values from 0 to 767, as said below
- tile_tgt: int32 [5120], P(('gx', 'gy')), may hold values from 0 to 1
- tile_count: int32 [32], P(('gx', 'gy')), may hold values from 128 to 160, as said below
- tile_weight: bfloat16 [5120, 256, 256], P(('gx', 'gy')), may hold values from -0.0625 to 0.0625
- ocean_state: bfloat16 [128, 128, 128], P('gy', 'gx'), may hold values from -6 to 6
- land_mask: int32 [128, 128], P('gy', 'gx'), may hold values 0 or 1
- mixing: float32 [128], replicated, may hold values from 0.03 to 0.24
Outputs:
- ocean_next: bfloat16 [128, 128, 128], P('gy', 'gx')
The draws below stay inside these ranges and needn't reach their ends.
Inputs may be any that keep to these rules, and one draw needn't show every extreme that they name: `atm_pos`: a permutation of the block positions. `tile_src`: among the 160 slots of one device, live or not, no owning device (atm_pos of the block // 24) is named by more than 8 slots; on every device with 160 live slots some owner is named by exactly 8. `tile_count`: live slots are a device's first ones; one device has exactly 160.
All inputs are finite; a program needn't handle non-finite values. No bound on the sum of `land_mask` on one device may be relied on, other than what follows from the above.
Results may differ from the reference program's by a relative error of at most 0.001.
Values may be sent and summed in bfloat16 or wider, within the bound.
No kernel may reach another device: no remote copies, remote signals or barrier semaphores. Data moves between devices by JAX's collectives and lax.ppermute only.
A program may use at most 128 MiB of HBM per device.

```python
import math
import jax
import jax.numpy as jnp
from jax import lax

TILE_ROWS = 256
CHANNELS = 128
ATM_BLOCKS = 24
TILE_SLOTS = 160
LAT_CELLS = 16
LON_CELLS = 32
RECV_SLOTS = 256
TARGET_BLOCKS = 2
ALL_BLOCKS = 768
ALL_TILES = 5120
LATITUDES = 128
LONGITUDES = 128
N_GX = 4
N_GY = 8
DEVICES = 32


def block_order(key):
    return jax.random.permutation(jax.random.fold_in(key, 11), ATM_BLOCKS * DEVICES).astype(jnp.int32)


def draw_atm_pos(key, part):
    return block_order(key)


def draw_tile_src(key, part):
    ordering = block_order(key)
    inverse = jnp.argsort(ordering, stable=True).astype(jnp.int32)
    per_peer = RECV_SLOTS // DEVICES
    device_keys = jax.random.split(jax.random.fold_in(key, 23), DEVICES)

    def one_device(device_key):
        first_key, second_key, third_key = jax.random.split(device_key, 3)
        owner_table = jax.random.permutation(first_key, DEVICES).astype(jnp.int32)
        owners = owner_table[jnp.arange(TILE_SLOTS, dtype=jnp.int32) // per_peer]
        owners = jax.random.permutation(second_key, owners)
        local_slot = jax.random.randint(third_key, (TILE_SLOTS,), 0, ATM_BLOCKS, dtype=jnp.int32)
        return inverse[owners * ATM_BLOCKS + local_slot]
    return jax.vmap(one_device)(device_keys).reshape(DEVICES * TILE_SLOTS).astype(jnp.int32)


def draw_tile_count(key, part):
    first_key, second_key = jax.random.split(jax.random.fold_in(key, 37))
    lowest = TILE_SLOTS - TILE_SLOTS // 5
    counts = jax.random.randint(first_key, (DEVICES,), lowest, TILE_SLOTS + 1, dtype=jnp.int32)
    busiest = jax.random.randint(second_key, (), 0, DEVICES, dtype=jnp.int32)
    return jnp.where(jnp.arange(DEVICES, dtype=jnp.int32) == busiest, TILE_SLOTS, counts).astype(jnp.int32)


def with_ends(entries, stream_key, least, largest):
    index_at = [jax.random.randint(jax.random.fold_in(stream_key, axis), (), 0, length) for axis, length in enumerate(entries.shape)]
    main_axis = entries.shape.index(max(entries.shape))
    beside = index_at[:main_axis] + [(index_at[main_axis] + 1) % entries.shape[main_axis]] + index_at[main_axis + 1:]
    return entries.at[tuple(index_at)].set(least).at[tuple(beside)].set(largest)


def level_of(key, shape, cuts, smallest, high):
    level, own = 1.0, jax.random.fold_in(key, 6)
    for axis_at, blocks in cuts:
        draws = jnp.exp(jax.random.uniform(jax.random.fold_in(own, axis_at), (blocks,), jnp.float32, smallest / len(cuts), high / len(cuts)))
        level = level * jnp.repeat(draws, shape[axis_at] // blocks).reshape([-1 if axis == axis_at else 1 for axis in range(len(shape))])
    return level


def bell_draw(stream_key, extent, width, bound, cuts=(), kind=jnp.bfloat16):
    entries = jax.random.normal(stream_key, extent, jnp.float32) * width
    if len(cuts) > 0:
        entries = level_of(stream_key, extent, cuts, -0.22, 0.18) * entries
    return jnp.clip(entries, min=-bound, max=bound).astype(kind)


def setup_inputs(seed: int = 0) -> dict:
    arg_keys = jax.random.split(jax.random.key(seed), 10)
    return {
        "atm_fields": bell_draw(arg_keys[0], (ALL_BLOCKS * TILE_ROWS, CHANNELS), 1.0, 6.0, ((0, 32),)),
        "atm_pos": draw_atm_pos(jax.random.fold_in(arg_keys[9], 71), 0),
        "tile_src": draw_tile_src(jax.random.fold_in(arg_keys[9], 71), 0),
        "tile_tgt": with_ends(jax.random.randint(arg_keys[3], (ALL_TILES,), 0, TARGET_BLOCKS), jax.random.fold_in(arg_keys[3], 1), 0, TARGET_BLOCKS - 1).astype(jnp.int32),
        "tile_count": draw_tile_count(jax.random.fold_in(arg_keys[9], 71), 0),
        "tile_weight": bell_draw(arg_keys[5], (ALL_TILES, TILE_ROWS, TILE_ROWS), (TILE_ROWS * TILE_SLOTS // 4) ** -0.5, 0.0625, ((0, 32),)),
        "ocean_state": bell_draw(arg_keys[6], (LATITUDES, LONGITUDES, CHANNELS), 1.0, 6.0, ((0, 8), (1, 4))),
        "land_mask": with_ends((jax.random.randint(arg_keys[7], (LATITUDES, LONGITUDES), 0, 4) < 3).astype(jnp.int32), jax.random.fold_in(arg_keys[7], 1), 0, 1),
        "mixing": jnp.clip(jnp.exp(jax.random.uniform(arg_keys[8], (CHANNELS,), jnp.float32, math.log(0.03), math.log(0.24))), 0.03, 0.24),
    }


def neighbours(field):
    west_side = jnp.roll(field, 1, axis=1)
    east_side = jnp.roll(field, -1, axis=1)
    south_side = jnp.concatenate([jnp.zeros_like(field[:1]), field[:-1]], axis=0)
    north_side = jnp.concatenate([field[1:], jnp.flip(field[-1:], axis=1)], axis=0)
    return (west_side, east_side, south_side, north_side)


def reference(atm_fields, atm_pos, tile_src, tile_tgt, tile_count, tile_weight, ocean_state, land_mask, mixing):
    devices = N_GX * N_GY
    block_table = atm_fields.reshape(ATM_BLOCKS * devices, TILE_ROWS, CHANNELS)

    def remap_device(pieces):
        weights, sources, targets, tile_live = pieces
        gathered = block_table[atm_pos[sources]].astype(jnp.float32)
        partial_sum = jnp.einsum("tij,tjc->tic", weights.astype(jnp.float32), gathered, precision=lax.Precision.HIGHEST)
        active = jnp.arange(TILE_SLOTS, dtype=jnp.int32) < tile_live
        select = ((targets[:, None] == jnp.arange(TARGET_BLOCKS, dtype=jnp.int32)[None, :]) & active[:, None]).astype(jnp.float32)
        summed = jnp.einsum("tb,tic->bic", select, partial_sum, precision=lax.Precision.HIGHEST)
        return summed.reshape(LAT_CELLS, LON_CELLS, CHANNELS)

    remapped = lax.map(remap_device, (tile_weight.reshape(devices, TILE_SLOTS, TILE_ROWS, TILE_ROWS), tile_src.reshape(devices, TILE_SLOTS), tile_tgt.reshape(devices, TILE_SLOTS), tile_count))
    forcing = remapped.reshape(N_GX, N_GY, LAT_CELLS, LON_CELLS, CHANNELS).transpose(1, 2, 0, 3, 4)
    forcing = forcing.reshape(N_GY * LAT_CELLS, N_GX * LON_CELLS, CHANNELS)
    center = ocean_state.astype(jnp.float32)
    wet_mask = land_mask.astype(jnp.float32)
    diffusion = jnp.zeros_like(center)
    for side_state, side_mask in zip(neighbours(center), neighbours(wet_mask)):
        diffusion = diffusion + side_mask[..., None] * (side_state - center)
    result = wet_mask[..., None] * (center + forcing + mixing * diffusion)
    return result.astype(jnp.bfloat16)
```

```python
import jax
import jax.numpy as jnp
from jax import lax
from jax.experimental import pallas as pl
from jax.experimental.pallas import tpu as pltpu
from jax.sharding import PartitionSpec as P

RECV_SLOTS = 256

STEP_TILES = 10
GATHER_LIMIT = 64 * 2**20


def tile_kernel(starts, place, target, weights, *refs):
    buffers, out, blocks, sems = refs[: len(starts)], refs[-3], refs[-2], refs[-1]
    group = weights.shape[0]
    step = pl.program_id(0)
    steps = pl.num_programs(0)

    def issue(at, slot):
        for j in range(group):
            where = place[at * group + j]
            for n, buffer in enumerate(buffers):
                first = starts[n]
                last = first + buffer.shape[0]

                @pl.when((where >= first) & (where < last))
                def _():
                    pltpu.make_async_copy(
                        buffer.at[where - first], blocks.at[slot, j], sems.at[slot, j]
                    ).start()

    @pl.when(step == 0)
    def _():
        out[...] = jnp.zeros_like(out)
        issue(0, 0)

    @pl.when(step + 1 < steps)
    def _():
        issue(step + 1, (step + 1) % 2)

    slot = step % 2
    for j in range(group):
        pltpu.make_async_copy(buffers[0].at[0], blocks.at[slot, j], sems.at[slot, j]).wait()
    for j in range(group):
        at = target[step * group + j]
        out[at] += jnp.dot(weights[j], blocks[slot, j], preferred_element_type=jnp.float32)


def remap(place, target, tile_weight, buffers, target_blocks):
    tiles, block_rows, _ = tile_weight.shape
    channels = buffers[0].shape[-1]
    group = max(d for d in range(1, STEP_TILES + 1) if tiles % d == 0)
    starts = []
    total = 0
    for buffer in buffers:
        starts.append(total)
        total += buffer.shape[0]

    def body(place_ref, target_ref, weights, *refs):
        tile_kernel(starts, place_ref, target_ref, weights, *refs)

    result = pl.pallas_call(
        body,
        grid_spec=pltpu.PrefetchScalarGridSpec(
            num_scalar_prefetch=2,
            grid=(tiles // group,),
            in_specs=[pl.BlockSpec((group, block_rows, block_rows), lambda i, *_: (i, 0, 0))]
            + [pl.BlockSpec(memory_space=pl.ANY)] * len(buffers),
            out_specs=pl.BlockSpec((target_blocks + 1, block_rows, channels), lambda i, *_: (0, 0, 0)),
            scratch_shapes=[
                pltpu.VMEM((2, group, block_rows, channels), jnp.bfloat16),
                pltpu.SemaphoreType.DMA((2, group)),
            ],
        ),
        out_shape=jax.ShapeDtypeStruct((target_blocks + 1, block_rows, channels), jnp.float32),
        compiler_params=pltpu.CompilerParams(dimension_semantics=("arbitrary",)),
    )(place, target, tile_weight, *buffers)
    return result[:target_blocks]


def padded(shard, sides, width, wrap):
    for axis, dim in sides:
        size, length = (lax.axis_size(axis), shard.shape[dim])
        up = [(i, (i + 1) % size) for i in range(size if wrap else size - 1)]
        down = [(j, i) for i, j in up]
        last = lax.slice_in_dim(shard, length - width, length, axis=dim)
        leading = lax.slice_in_dim(shard, 0, width, axis=dim)
        before = lax.ppermute(last, axis, up)
        after = lax.ppermute(leading, axis, down)
        shard = jnp.concatenate([before, shard, after], axis=dim)
    return shard


def partner(value, axis, distance):
    mask = 2**distance
    pairs = [(source, source ^ mask) for source in range(lax.axis_size(axis))]
    return lax.ppermute(value, axis, pairs)


def plan_tiles(sources, tile_live, atm_pos, block_count):
    positions = atm_pos[sources]
    owners = positions // block_count
    local_slot = positions % block_count
    ordinal = jnp.arange(sources.shape[0], dtype=jnp.int32)
    active = ordinal < tile_live
    earlier = (
        (owners[:, None] == owners[None, :])
        & active[None, :]
        & (ordinal[None, :] < ordinal[:, None])
    )
    order_rank = jnp.sum(earlier.astype(jnp.int32), axis=1)
    return (owners, order_rank, local_slot, active)


def exchanged_blocks(block_table, tile_src, tile_live, atm_pos):
    block_count, block_rows, channels = block_table.shape
    devices = lax.axis_size("gx") * lax.axis_size("gy")
    per_peer = RECV_SLOTS // devices
    owners, order_rank, local_slot, active = plan_tiles(tile_src, tile_live, atm_pos, block_count)
    slots_flat = jnp.arange(RECV_SLOTS, dtype=jnp.int32)
    wanted_slot = owners * per_peer + order_rank
    matches = (wanted_slot[None, :] == slots_flat[:, None]) & active[None, :]
    asking = jnp.sum(jnp.where(matches, local_slot[None, :], 0), axis=1)
    requests = lax.all_to_all(
        asking.reshape(devices, per_peer), ("gx", "gy"), split_axis=0, concat_axis=0, tiled=True
    )
    outgoing = block_table[requests.reshape(RECV_SLOTS)]
    outgoing = outgoing.reshape(devices, per_peer, block_rows, channels)
    arrived = lax.all_to_all(outgoing, ("gx", "gy"), split_axis=0, concat_axis=0, tiled=True)
    arrived = arrived.reshape(RECV_SLOTS, block_rows, channels)
    return jnp.where(active, wanted_slot, 0), [arrived]


def gathered_blocks(block_table, positions):
    return positions, [lax.all_gather(block_table, ("gx", "gy"), tiled=True)]


def local(
    atm_fields, atm_pos, tile_src, tile_tgt, tile_count, tile_weight, ocean_state, land_mask, mixing
):
    block_rows = tile_weight.shape[1]
    tiles = tile_weight.shape[0]
    channels = atm_fields.shape[1]
    block_count = atm_fields.shape[0] // block_rows
    devices = lax.axis_size("gx") * lax.axis_size("gy")
    lat_rows = ocean_state.shape[0]
    lon_cols = ocean_state.shape[1]
    target_blocks = lat_rows * lon_cols // block_rows
    block_table = atm_fields.reshape(block_count, block_rows, channels)
    active = jnp.arange(tiles, dtype=jnp.int32) < tile_count[0]
    target = jnp.where(active, tile_tgt, target_blocks)
    if devices * atm_fields.size * atm_fields.dtype.itemsize <= GATHER_LIMIT:
        place, buffers = gathered_blocks(block_table, atm_pos[tile_src])
    else:
        place, buffers = exchanged_blocks(block_table, tile_src, tile_count[0], atm_pos)
    remapped = remap(place, target, tile_weight, buffers, target_blocks)
    forcing = remapped.reshape(lat_rows, lon_cols, channels)
    mask_half = land_mask.astype(jnp.bfloat16)
    lon_state, lon_mask = (
        padded(ocean_state, (("gx", 1),), 1, True),
        padded(mask_half, (("gx", 1),), 1, True),
    )
    lat_state, lat_mask = (
        padded(ocean_state, (("gy", 0),), 1, False),
        padded(mask_half, (("gy", 0),), 1, False),
    )
    fold_state = jnp.flip(ocean_state[-1], 0)
    fold_mask = jnp.flip(mask_half[-1], 0)
    for bit_number in range(lax.axis_size("gx").bit_length() - 1):
        fold_state, fold_mask = partner((fold_state, fold_mask), "gx", bit_number)
    is_top = lax.axis_index("gy") == lax.axis_size("gy") - 1
    north_state = jnp.concatenate(
        [lat_state[2:-1], jnp.where(is_top, fold_state, lat_state[-1])[None]], axis=0
    )
    north_mask = jnp.concatenate(
        [lat_mask[2:-1], jnp.where(is_top, fold_mask, lat_mask[-1])[None]], axis=0
    )
    center = ocean_state.astype(jnp.float32)
    sides = (
        (lon_state[:, :-2], lon_mask[:, :-2]),
        (lon_state[:, 2:], lon_mask[:, 2:]),
        (lat_state[:-2], lat_mask[:-2]),
        (north_state, north_mask),
    )
    diffusion = jnp.zeros_like(center)
    for side_state, side_mask in sides:
        diffusion = diffusion + side_mask.astype(jnp.float32)[..., None] * (
            side_state.astype(jnp.float32) - center
        )
    result = mask_half.astype(jnp.float32)[..., None] * (center + forcing + mixing * diffusion)
    return result.astype(jnp.bfloat16)


def solution(mesh):
    in_specs = (
        P(("gx", "gy"), None),
        P(),
        P(("gx", "gy")),
        P(("gx", "gy")),
        P(("gx", "gy")),
        P(("gx", "gy"), None, None),
        P("gy", "gx", None),
        P("gy", "gx"),
        P(),
    )
    out_specs = P("gy", "gx", None)
    return jax.shard_map(local, mesh=mesh, in_specs=in_specs, out_specs=out_specs, check_vma=False)
```

```python
import jax
import jax.numpy as jnp
import numpy as np
from jax import lax
from jax.experimental import pallas as pl
from jax.experimental.pallas import tpu as pltpu
from jax.sharding import PartitionSpec as P

RECV_SLOTS = 256

STEP_TILES = 10
GATHER_LIMIT = 64 * 2**20


def tile_kernel(starts, place, target, weights, *refs):
    buffers, out, blocks, sems = refs[: len(starts)], refs[-3], refs[-2], refs[-1]
    group = weights.shape[0]
    step = pl.program_id(0)
    steps = pl.num_programs(0)

    def issue(at, slot):
        for j in range(group):
            where = place[at * group + j]
            for n, buffer in enumerate(buffers):
                first = starts[n]
                last = first + buffer.shape[0]

                @pl.when((where >= first) & (where < last))
                def _():
                    pltpu.make_async_copy(
                        buffer.at[where - first], blocks.at[slot, j], sems.at[slot, j]
                    ).start()

    @pl.when(step == 0)
    def _():
        out[...] = jnp.zeros_like(out)
        issue(0, 0)

    @pl.when(step + 1 < steps)
    def _():
        issue(step + 1, (step + 1) % 2)

    slot = step % 2
    for j in range(group):
        pltpu.make_async_copy(buffers[0].at[0], blocks.at[slot, j], sems.at[slot, j]).wait()
    for j in range(group):
        at = target[step * group + j]
        out[at] += jnp.dot(weights[j], blocks[slot, j], preferred_element_type=jnp.float32)


def remap(place, target, tile_weight, buffers, target_blocks):
    tiles, block_rows, _ = tile_weight.shape
    channels = buffers[0].shape[-1]
    group = max(d for d in range(1, STEP_TILES + 1) if tiles % d == 0)
    starts = []
    total = 0
    for buffer in buffers:
        starts.append(total)
        total += buffer.shape[0]

    def body(place_ref, target_ref, weights, *refs):
        tile_kernel(starts, place_ref, target_ref, weights, *refs)

    result = pl.pallas_call(
        body,
        grid_spec=pltpu.PrefetchScalarGridSpec(
            num_scalar_prefetch=2,
            grid=(tiles // group,),
            in_specs=[pl.BlockSpec((group, block_rows, block_rows), lambda i, *_: (i, 0, 0))]
            + [pl.BlockSpec(memory_space=pl.ANY)] * len(buffers),
            out_specs=pl.BlockSpec((target_blocks + 1, block_rows, channels), lambda i, *_: (0, 0, 0)),
            scratch_shapes=[
                pltpu.VMEM((2, group, block_rows, channels), jnp.bfloat16),
                pltpu.SemaphoreType.DMA((2, group)),
            ],
        ),
        out_shape=jax.ShapeDtypeStruct((target_blocks + 1, block_rows, channels), jnp.float32),
        compiler_params=pltpu.CompilerParams(dimension_semantics=("arbitrary",)),
    )(place, target, tile_weight, *buffers)
    return result[:target_blocks]


def padded(shard, sides, width, wrap):
    for axis, dim in sides:
        size, length = (lax.axis_size(axis), shard.shape[dim])
        up = [(i, (i + 1) % size) for i in range(size if wrap else size - 1)]
        down = [(j, i) for i, j in up]
        last = lax.slice_in_dim(shard, length - width, length, axis=dim)
        leading = lax.slice_in_dim(shard, 0, width, axis=dim)
        before = lax.ppermute(last, axis, up)
        after = lax.ppermute(leading, axis, down)
        shard = jnp.concatenate([before, shard, after], axis=dim)
    return shard


def partner(value, axis, distance):
    mask = 2**distance
    pairs = [(source, source ^ mask) for source in range(lax.axis_size(axis))]
    return lax.ppermute(value, axis, pairs)


def plan_tiles(sources, tile_live, atm_pos, block_count):
    positions = atm_pos[sources]
    owners = positions // block_count
    local_slot = positions % block_count
    ordinal = jnp.arange(sources.shape[0], dtype=jnp.int32)
    active = ordinal < tile_live
    earlier = (
        (owners[:, None] == owners[None, :])
        & active[None, :]
        & (ordinal[None, :] < ordinal[:, None])
    )
    order_rank = jnp.sum(earlier.astype(jnp.int32), axis=1)
    return (owners, order_rank, local_slot, active)


def exchanged_blocks(block_table, tile_src, tile_live, atm_pos):
    block_count, block_rows, channels = block_table.shape
    devices = lax.axis_size("gx") * lax.axis_size("gy")
    per_peer = RECV_SLOTS // devices
    owners, order_rank, local_slot, active = plan_tiles(tile_src, tile_live, atm_pos, block_count)
    slots_flat = jnp.arange(RECV_SLOTS, dtype=jnp.int32)
    wanted_slot = owners * per_peer + order_rank
    matches = (wanted_slot[None, :] == slots_flat[:, None]) & active[None, :]
    asking = jnp.sum(jnp.where(matches, local_slot[None, :], 0), axis=1)
    requests = lax.all_to_all(
        asking.reshape(devices, per_peer), ("gx", "gy"), split_axis=0, concat_axis=0, tiled=True
    )
    outgoing = block_table[requests.reshape(RECV_SLOTS)]
    outgoing = outgoing.reshape(devices, per_peer, block_rows, channels)
    arrived = lax.all_to_all(outgoing, ("gx", "gy"), split_axis=0, concat_axis=0, tiled=True)
    arrived = arrived.reshape(RECV_SLOTS, block_rows, channels)
    return jnp.where(active, wanted_slot, 0), [arrived]


def link_sizes():
    gx, gy = lax.axis_size("gx"), lax.axis_size("gy")
    ny = 2 ** ((gy.bit_length() - 1) // 2)
    return gx // 2, 2, gy // ny, ny


def shifted(value, dx=0, dc=0, dz=0, dy=0):
    nx, nc, nz, ny = link_sizes()
    pairs = []
    for source in range(nx * nc * nz * ny):
        x, c, z, y = np.unravel_index(source, (nx, nc, nz, ny))
        to = ((x + dx) % nx, (c + dc) % nc, (z + dz) % nz, (y + dy) % ny)
        pairs.append((source, int(np.ravel_multi_index(to, (nx, nc, nz, ny)))))
    return lax.ppermute(value, ("gx", "gy"), pairs)


def tags_moved(tags, nz, dx=0, dc=0, dz=0, dy=0):
    return [(x ^ dx, c ^ dc, (z + dz) % nz, y ^ dy, slot) for x, c, z, y, slot in tags]


def gathered_blocks(block_table, positions):
    nx, nc, nz, ny = link_sizes()
    count = block_table.shape[0]
    if nx != 2 or ny != 2:
        return positions, [lax.all_gather(block_table, ("gx", "gy"), tiled=True)]
    half = count * 5 // 12

    def move(piece, **by):
        return shifted(piece[0], **by), tags_moved(piece[1], nz, **by)

    def join(*pieces):
        return jnp.concatenate([p[0] for p in pieces]), sum([p[1] for p in pieces], [])

    def cut(piece, low, high):
        return piece[0][low:high], piece[1][low:high]

    own = (block_table, [(0, 0, 0, 0, slot) for slot in range(count)])
    late = cut(own, 2 * half, count)
    early = cut(own, 0, 2 * half)
    late = join(late, move(late, dx=1))
    late = join(late, move(late, dy=1))
    groups = []
    for k in range(nz):
        if k > 0:
            early = move(early, dz=1)
        first, second = cut(early, 0, half), cut(early, half, 2 * half)
        first = join(first, move(first, dx=1))
        second = join(second, move(second, dy=1))
        groups.append(join(first, second, move(first, dy=1), move(second, dx=1)))
    ring = [late]
    for k in range(1, nz):
        ring.append(move(ring[-1], dz=1))
    groups.insert(nz - 1, join(*ring))
    groups = groups + [move(g, dc=1) for g in groups]
    table = np.zeros((nx, nc, nz, ny, count), np.int32)
    at = 0
    for _, tags in groups:
        for tag in tags:
            table[tag] = at
            at += 1
    my_x, my_c = lax.axis_index("gx") // nc, lax.axis_index("gx") % nc
    my_z, my_y = lax.axis_index("gy") // ny, lax.axis_index("gy") % ny
    owner, slot = positions // count, positions % count
    y = (my_y - owner % ny) % ny
    z = (my_z - owner // ny % nz) % nz
    c = (my_c - owner // (ny * nz) % nc) % nc
    x = (my_x - owner // (ny * nz * nc)) % nx
    relative = (((x * nc + c) * nz + z) * ny + y) * count + slot
    return jnp.asarray(table.reshape(-1))[relative], [g[0] for g in groups]


def local(
    atm_fields, atm_pos, tile_src, tile_tgt, tile_count, tile_weight, ocean_state, land_mask, mixing
):
    block_rows = tile_weight.shape[1]
    tiles = tile_weight.shape[0]
    channels = atm_fields.shape[1]
    block_count = atm_fields.shape[0] // block_rows
    devices = lax.axis_size("gx") * lax.axis_size("gy")
    lat_rows = ocean_state.shape[0]
    lon_cols = ocean_state.shape[1]
    target_blocks = lat_rows * lon_cols // block_rows
    block_table = atm_fields.reshape(block_count, block_rows, channels)
    active = jnp.arange(tiles, dtype=jnp.int32) < tile_count[0]
    target = jnp.where(active, tile_tgt, target_blocks)
    if devices * atm_fields.size * atm_fields.dtype.itemsize <= GATHER_LIMIT:
        place, buffers = gathered_blocks(block_table, atm_pos[tile_src])
    else:
        place, buffers = exchanged_blocks(block_table, tile_src, tile_count[0], atm_pos)
    remapped = remap(place, target, tile_weight, buffers, target_blocks)
    forcing = remapped.reshape(lat_rows, lon_cols, channels)
    mask_half = land_mask.astype(jnp.bfloat16)
    lon_state, lon_mask = (
        padded(ocean_state, (("gx", 1),), 1, True),
        padded(mask_half, (("gx", 1),), 1, True),
    )
    lat_state, lat_mask = (
        padded(ocean_state, (("gy", 0),), 1, False),
        padded(mask_half, (("gy", 0),), 1, False),
    )
    fold_state = jnp.flip(ocean_state[-1], 0)
    fold_mask = jnp.flip(mask_half[-1], 0)
    for bit_number in range(lax.axis_size("gx").bit_length() - 1):
        fold_state, fold_mask = partner((fold_state, fold_mask), "gx", bit_number)
    is_top = lax.axis_index("gy") == lax.axis_size("gy") - 1
    north_state = jnp.concatenate(
        [lat_state[2:-1], jnp.where(is_top, fold_state, lat_state[-1])[None]], axis=0
    )
    north_mask = jnp.concatenate(
        [lat_mask[2:-1], jnp.where(is_top, fold_mask, lat_mask[-1])[None]], axis=0
    )
    center = ocean_state.astype(jnp.float32)
    sides = (
        (lon_state[:, :-2], lon_mask[:, :-2]),
        (lon_state[:, 2:], lon_mask[:, 2:]),
        (lat_state[:-2], lat_mask[:-2]),
        (north_state, north_mask),
    )
    diffusion = jnp.zeros_like(center)
    for side_state, side_mask in sides:
        diffusion = diffusion + side_mask.astype(jnp.float32)[..., None] * (
            side_state.astype(jnp.float32) - center
        )
    result = mask_half.astype(jnp.float32)[..., None] * (center + forcing + mixing * diffusion)
    return result.astype(jnp.bfloat16)


def solution(mesh):
    in_specs = (
        P(("gx", "gy"), None),
        P(),
        P(("gx", "gy")),
        P(("gx", "gy")),
        P(("gx", "gy")),
        P(("gx", "gy"), None, None),
        P("gy", "gx", None),
        P("gy", "gx"),
        P(),
    )
    out_specs = P("gy", "gx", None)
    return jax.shard_map(local, mesh=mesh, in_specs=in_specs, out_specs=out_specs, check_vma=False)
```
